32 devices in a mesh: groups: 2 (over y), cache: 4 (over x, core), tensor: 4 (over z).
Axes of the slice: x: 2, y: 2, z: 4, core: 2. Of those that a mesh axis runs over, the one named last changes fastest.
Arguments:
- queries: bfloat16 [2048, 8192], P(('groups', 'cache'), 'tensor'), parts along dimension 0, may hold values from -8 to 8
- suffix_key_value: bfloat16 [2, 2048, 1024], P(None, ('groups', 'cache'), 'tensor'), parts along dimension 1, may hold values from -6 to 6
- kv_pages: bfloat16 [768, 2, 128, 1024], P(('groups', 'cache'), None, None, 'tensor'), parts along dimension 0, may hold values from -6 to 6
- page_ids: int32 [8, 64], P(('groups', 'cache')), parts along dimension 0, may hold values from 0 to 383, as said below
- prefix_pages: int32 [8], P(('groups', 'cache')), parts along dimension 0, may hold values from 8 to 64, as said below
- page_home: int32 [768], P('groups'), parts along dimension 0, may hold values from 0 to 383, as said below
- out_weight: bfloat16 [8192, 8192], P('tensor', 'cache'), may hold values from -0.25 to 0.25
Outputs:
- attended: bfloat16 [2048, 8192], P(('groups', 'cache'), 'tensor'), parts along dimension 0
The draws below stay inside these ranges and needn't reach their ends.
There are 2 independent parts, one for each index of `groups`. The reference program is written for one: setup_inputs(seed, part) draws one part's arguments, and reference() takes and returns one part's arrays. A program takes and returns all parts, laid end to end along the dimension named above; an argument that names none is the same for every part. Nothing has to cross between parts.
Inputs may be any that keep to these rules, and one draw needn't show every extreme that they name: `page_ids`: live slots are j < prefix_pages[r]. Within the aligned block of 1 request of one index of cache, no page id appears twice among all 64 slots, and at most 24 of these slots name pages whose row page_home[id] lies on one index of cache (row // 96); in every such block some index of cache gets exactly 24. `prefix_pages`: one request in each draw has 64 pages and another has 8. `page_home`: A permutation of 0 to 383.
All inputs are finite; a program needn't handle non-finite values.
Results may differ from the reference program's by a relative error of at most 0.015.
Values may be sent and summed in bfloat16 or wider, within the bound.
No kernel may reach another device: no remote copies, remote signals or barrier semaphores. Data moves between devices by JAX's collectives and lax.ppermute only.
A program may use at most 128 MiB of HBM per device.

```python
import jax
import jax.numpy as jnp
from jax import lax

D = 8192
QUERY_HEADS = 64
KEY_VALUE_HEADS = 8
HEAD_SIZE = 128
PAGE_TOKENS = 128
SUF = 256
MAXP = 64
MINP = 8
POOL_DEV = 96
REQ_DEV = 1
REQS = 4
NEW_TOKENS = 1024
STORED_PAGES = 384
CAP = 24
N_CACHE = 4
N_TENSOR = 4


def page_layout(key):
    base_key = jax.random.fold_in(key, 7001)
    home_rows = jax.random.permutation(jax.random.fold_in(base_key, 1), STORED_PAGES).astype(jnp.int32)
    inverse = jnp.zeros((STORED_PAGES,), jnp.int32).at[home_rows].set(jnp.arange(STORED_PAGES, dtype=jnp.int32))
    slot_count = REQ_DEV * MAXP

    def one_device(device):
        device_key = jax.random.fold_in(base_key, 100 + device)
        remaining = jax.random.permutation(jax.random.fold_in(device_key, 1), N_CACHE * CAP - CAP).astype(jnp.int32) + CAP
        tickets = jnp.concatenate([jnp.arange(CAP, dtype=jnp.int32), remaining])[:slot_count]
        shuffle = jax.random.permutation(jax.random.fold_in(device_key, 2), slot_count)
        tickets = tickets[shuffle]
        first_owner = jax.random.randint(jax.random.fold_in(device_key, 3), (), 0, N_CACHE)
        owners = (tickets // CAP + first_owner) % N_CACHE
        offset = jax.random.randint(jax.random.fold_in(device_key, 4), (N_CACHE,), 0, POOL_DEV)
        within = (offset[owners] + tickets % CAP) % POOL_DEV
        return inverse[owners * POOL_DEV + within]
    page_list = jax.vmap(one_device)(jnp.arange(N_CACHE, dtype=jnp.int32))
    return (home_rows, page_list.reshape(N_CACHE * REQ_DEV, MAXP).astype(jnp.int32))


def draw_page_home(key, part):
    return page_layout(key)[0]


def draw_page_ids(key, part):
    return page_layout(key)[1]


def draw_prefix_pages(key, part):
    base_key = jax.random.fold_in(key, 7002)
    length_span = MAXP - MINP
    first_draw = jax.random.randint(jax.random.fold_in(base_key, 1), (REQS,), 0, length_span + 1)
    second_draw = jax.random.randint(jax.random.fold_in(base_key, 2), (REQS,), 0, length_span + 1)
    lengths = MAXP - first_draw * second_draw // max(length_span, 1)
    longest = jax.random.randint(jax.random.fold_in(base_key, 3), (), 0, REQS)
    step_away = jax.random.randint(jax.random.fold_in(base_key, 4), (), 1, max(REQS, 2))
    shortest = (longest + step_away) % REQS
    request_index = jnp.arange(REQS)
    lengths = jnp.where(request_index == shortest, MINP, lengths)
    lengths = jnp.where(request_index == longest, MAXP, lengths)
    return lengths.astype(jnp.int32)


def draw_queries(key, part):
    noise_key = jax.random.fold_in(key, 7004)
    values = jnp.clip(2.5 * jax.random.normal(noise_key, (NEW_TOKENS, QUERY_HEADS * HEAD_SIZE), jnp.float32), -8.0, 8.0)
    return values.astype(jnp.bfloat16)


def draw_kv_pages(key, part):
    noise_key = jax.random.fold_in(key, 7005)
    array_shape = (STORED_PAGES, 2, PAGE_TOKENS, KEY_VALUE_HEADS * HEAD_SIZE)
    values = jnp.clip(jax.random.normal(noise_key, array_shape, jnp.float32), -6.0, 6.0)
    return values.astype(jnp.bfloat16)


def steps_of(rng, extent, cuts, low, top_value):
    loudness, own = 1.0, jax.random.fold_in(rng, 6)
    for dim, parts in cuts:
        heights = jnp.exp(jax.random.uniform(jax.random.fold_in(own, dim), (parts,), jnp.float32, low / len(cuts), top_value / len(cuts)))
        loudness = loudness * jnp.repeat(heights, extent[dim] // parts).reshape([-1 if axis == dim else 1 for axis in range(len(extent))])
    return loudness


def gaussian(stream_key, extent, scale, most, shards=(), kind=jnp.bfloat16):
    result = scale * jax.random.normal(stream_key, extent, jnp.float32)
    if shards:
        result = result * steps_of(stream_key, extent, shards, -0.22, 0.18)
    return jnp.clip(result, -most, most).astype(kind)


def setup_inputs(seed: int = 0, part: int = 0) -> dict:
    streams_of = jax.random.split(jax.random.key(seed), 8)
    own_keys = jax.random.split(jax.random.fold_in(streams_of[7], part), 8)
    return {
        "queries": draw_queries(jax.random.fold_in(jax.random.fold_in(streams_of[7], part), 71), part),
        "suffix_key_value": gaussian(own_keys[1], (2, NEW_TOKENS, KEY_VALUE_HEADS * HEAD_SIZE), 1.0, 6.0, ((1, 4), (2, 4))),
        "kv_pages": draw_kv_pages(jax.random.fold_in(jax.random.fold_in(streams_of[7], part), 71), part),
        "page_ids": draw_page_ids(jax.random.fold_in(jax.random.fold_in(streams_of[7], part), 71), part),
        "prefix_pages": draw_prefix_pages(jax.random.fold_in(jax.random.fold_in(streams_of[7], part), 71), part),
        "page_home": draw_page_home(jax.random.fold_in(jax.random.fold_in(streams_of[7], part), 71), part),
        "out_weight": gaussian(streams_of[6], (QUERY_HEADS * HEAD_SIZE, D), (QUERY_HEADS * HEAD_SIZE // 16) ** -0.5, 0.25, ((0, 4), (1, 4))),
    }


def attend_head(query_head, key_rows, value_rows, allowed):
    scores = jnp.einsum("sgd,ld->sgl", query_head.astype(jnp.float32), key_rows.astype(jnp.float32)) * (HEAD_SIZE ** -0.5)
    scores = jnp.where(allowed[:, None, :], scores, -jnp.inf)
    row_top = jnp.max(scores, axis=2, keepdims=True)
    weights = jnp.where(allowed[:, None, :], jnp.exp(scores - row_top), 0.0)
    weight_sum = jnp.sum(weights, axis=2, keepdims=True)
    rounded = lax.optimization_barrier(weights.astype(jnp.bfloat16))
    accumulated = jnp.einsum("sgl,ld->sgd", rounded.astype(jnp.float32), value_rows.astype(jnp.float32))
    return (accumulated / weight_sum).astype(jnp.bfloat16)


def reference(queries, suffix_key_value, kv_pages, page_ids, prefix_pages, page_home, out_weight):
    group_width = QUERY_HEADS // KEY_VALUE_HEADS

    def one_request(request_index):
        page_list = page_ids[request_index]
        home_rows = jnp.take(page_home, page_list).astype(jnp.int32)
        pages_here = jnp.take(kv_pages, home_rows, axis=0)
        first_token = (request_index * SUF).astype(jnp.int32)
        query_rows = lax.dynamic_slice_in_dim(queries, first_token, SUF, 0)
        suffix_rows = lax.dynamic_slice_in_dim(suffix_key_value, first_token, SUF, 1)
        key_page = jnp.arange(MAXP * PAGE_TOKENS, dtype=jnp.int32) // PAGE_TOKENS
        prefix_live = jnp.broadcast_to((key_page < prefix_pages[request_index])[None, :], (SUF, MAXP * PAGE_TOKENS))
        positions = jnp.arange(SUF, dtype=jnp.int32)
        causal = positions[None, :] <= positions[:, None]
        allowed = jnp.concatenate([prefix_live, causal], axis=1)

        def single_head(head_index):
            query_head = lax.dynamic_slice_in_dim(query_rows, (head_index * group_width * HEAD_SIZE).astype(jnp.int32), group_width * HEAD_SIZE, 1)
            query_head = query_head.reshape(SUF, group_width, HEAD_SIZE)
            column = (head_index * HEAD_SIZE).astype(jnp.int32)
            prefix_keys = lax.dynamic_slice_in_dim(pages_here[:, 0], column, HEAD_SIZE, 2).reshape(MAXP * PAGE_TOKENS, HEAD_SIZE)
            prefix_values = lax.dynamic_slice_in_dim(pages_here[:, 1], column, HEAD_SIZE, 2).reshape(MAXP * PAGE_TOKENS, HEAD_SIZE)
            suffix_keys = lax.dynamic_slice_in_dim(suffix_rows[0], column, HEAD_SIZE, 1)
            suffix_values = lax.dynamic_slice_in_dim(suffix_rows[1], column, HEAD_SIZE, 1)
            key_rows = jnp.concatenate([prefix_keys, suffix_keys], axis=0)
            value_rows = jnp.concatenate([prefix_values, suffix_values], axis=0)
            return attend_head(query_head, key_rows, value_rows, allowed)

        head_list = lax.map(single_head, jnp.arange(KEY_VALUE_HEADS, dtype=jnp.int32))
        return jnp.transpose(head_list, (1, 0, 2, 3)).reshape(SUF, QUERY_HEADS * HEAD_SIZE)

    mixed_heads = lax.map(one_request, jnp.arange(REQS, dtype=jnp.int32)).reshape(NEW_TOKENS, QUERY_HEADS * HEAD_SIZE)
    span_cols = QUERY_HEADS * HEAD_SIZE // N_TENSOR
    summed = jnp.zeros((NEW_TOKENS, D), jnp.float32)
    for group_index in range(N_TENSOR):
        lower = group_index * span_cols
        group_term = jnp.dot(mixed_heads[:, lower:lower + span_cols], out_weight[lower:lower + span_cols], preferred_element_type=jnp.float32).astype(jnp.bfloat16)
        summed = summed + lax.optimization_barrier(group_term).astype(jnp.float32)
    return summed.astype(jnp.bfloat16)
```

```python
import functools

import jax
import jax.numpy as jnp
from jax import lax
from jax.experimental import pallas as pl
from jax.experimental.pallas import tpu as pltpu
from jax.sharding import PartitionSpec as P


HEAD_SIZE = 128

nothing = -1e30
pages_per_block = 4
token_pieces = 2
log2_e = 1.4426950408889634


def attend_kernel(which, lists, counts, token, *refs, parts, kv_heads, heads, tokens, first_token, suffix):
    queries, refs = refs[:parts], refs[parts:]
    pages, refs = refs[0], refs[1:]
    if suffix:
        suffix_kv, refs = refs[0], refs[1:]
    outs, lses, refs = refs[:parts], refs[parts : 2 * parts], refs[2 * parts :]
    q, q_sems, buf, sems, top_s, sum_s, acc_s = refs
    page_tokens = pages.shape[2]
    rows = heads * tokens
    factor = HEAD_SIZE ** (-0.5) * log2_e
    block_keys = pages_per_block * page_tokens

    def live_of(part):
        return counts[which[part]]

    def blocks_of(part):
        return (live_of(part) + pages_per_block - 1) // pages_per_block

    def copy_of(part, block, slot, place):
        row = lists[which[part], block * pages_per_block + place]
        return pltpu.make_async_copy(pages.at[row], buf.at[slot, place], sems.at[slot, place])

    def start(part, block, slot):
        for place in range(pages_per_block):
            copy_of(part, block, slot, place).start()

    def query_copy(part):
        return pltpu.make_async_copy(queries[part], q.at[part], q_sems.at[part])

    for part in range(parts):
        query_copy(part).start()

    def queries_of(part, kv_head):
        head = kv_head * heads
        return jnp.concatenate(
            [
                q[part, :, (head + i) * HEAD_SIZE : (head + i + 1) * HEAD_SIZE]
                for i in range(heads)
            ],
            axis=0,
        )

    def lane_tiles(x):
        return [x[:, i : i + HEAD_SIZE] for i in range(0, x.shape[1], HEAD_SIZE)]

    def step(part, kv_head, keys, values, mask, first):
        s = lax.dot_general(
            queries_of(part, kv_head),
            keys,
            (((1,), (1,)), ((), ())),
            preferred_element_type=jnp.float32,
        )
        s = mask(s)
        tops = functools.reduce(jnp.maximum, lane_tiles(s))
        top = jnp.broadcast_to(jnp.max(tops, axis=1, keepdims=True), (rows, HEAD_SIZE))
        if not first:
            before = top_s[kv_head]
            top = jnp.maximum(before, top)
            alpha = jnp.exp2((before - top) * factor)
        weights = [jnp.exp2((tile - top) * factor) for tile in lane_tiles(s)]
        sums = functools.reduce(jnp.add, weights)
        product = lax.dot_general(
            jnp.concatenate([w.astype(jnp.bfloat16) for w in weights], axis=1),
            values,
            (((1,), (0,)), ((), ())),
            preferred_element_type=jnp.float32,
        )
        top_s[kv_head] = top
        if first:
            sum_s[kv_head] = sums
            acc_s[kv_head] = product
        else:
            sum_s[kv_head] = sum_s[kv_head] * alpha + sums
            acc_s[kv_head] = acc_s[kv_head] * alpha + product

    def columns_of(kv_head):
        return slice(kv_head * HEAD_SIZE, (kv_head + 1) * HEAD_SIZE)

    def begin_suffix():
        def causal(s):
            token = lax.broadcasted_iota(jnp.int32, s.shape, 0) % tokens + first_token
            key = lax.broadcasted_iota(jnp.int32, s.shape, 1)
            return jnp.where(key <= token, s, nothing)

        keys = slice(0, first_token + tokens)
        for kv_head in range(kv_heads):
            columns = columns_of(kv_head)
            step(0, kv_head, suffix_kv[0, keys, columns], suffix_kv[1, keys, columns], causal, True)

    def begin_empty():
        top_s[...] = jnp.full(top_s.shape, nothing, jnp.float32)
        sum_s[...] = jnp.zeros(sum_s.shape, jnp.float32)
        acc_s[...] = jnp.zeros(acc_s.shape, jnp.float32)

    def part_step(part, carry):
        base, started = carry
        blocks = blocks_of(part)
        after = jnp.minimum(part + 1, parts - 1)
        more = (part + 1 < parts) & (blocks_of(after) > 0)

        @pl.when((blocks > 0) & jnp.logical_not(started))
        def _():
            start(part, 0, lax.rem(base, 2))

        for i in range(parts):

            @pl.when(part == i)
            def _():
                query_copy(i).wait()

        if suffix:
            pl.when(part == 0)(begin_suffix)
            pl.when(part != 0)(begin_empty)
        else:
            begin_empty()

        def block_step(block, carry):
            slot = lax.rem(base + block, 2)
            last = block + 1 == blocks

            @pl.when(jnp.logical_not(last) | more)
            def _():
                start(jnp.where(last, after, part), jnp.where(last, 0, block + 1), 1 - slot)

            for place in range(pages_per_block):
                copy_of(part, block, slot, place).wait()
            key = lax.broadcasted_iota(jnp.int32, (1, block_keys), 1)
            left = (live_of(part) - block * pages_per_block) * page_tokens
            bias = jnp.where(key < left, 0.0, nothing)
            for kv_head in range(kv_heads):
                keys = buf[slot, :, 0, :, columns_of(kv_head)].reshape(block_keys, HEAD_SIZE)
                values = buf[slot, :, 1, :, columns_of(kv_head)].reshape(block_keys, HEAD_SIZE)
                step(part, kv_head, keys, values, lambda s: s + bias, False)
            return carry

        lax.fori_loop(0, blocks, block_step, 0)

        lane = lax.broadcasted_iota(jnp.int32, (tokens, HEAD_SIZE), 1)
        packed = jnp.zeros((tokens, HEAD_SIZE), jnp.float32)
        for kv_head in range(kv_heads):
            total = jnp.sum(sum_s[kv_head], axis=1, keepdims=True)
            any_key = total > 0.0
            safe = jnp.where(any_key, total, 1.0)
            acc_s[kv_head] = acc_s[kv_head] * (1.0 / safe)
            stat = jnp.where(any_key, top_s[kv_head] * factor + jnp.log2(safe), nothing)
            for i in range(heads):
                packed = jnp.where(
                    lane == kv_head * heads + i, stat[i * tokens : (i + 1) * tokens], packed
                )
        packed = packed.T[: kv_heads * heads]
        for i in range(parts):

            @pl.when(part == i)
            def _():
                lses[i][...] = packed
                for kv_head in range(kv_heads):
                    for j in range(heads):
                        head = kv_head * heads + j
                        outs[i][:, head * HEAD_SIZE : (head + 1) * HEAD_SIZE] = acc_s[
                            kv_head, j * tokens : (j + 1) * tokens
                        ].astype(jnp.bfloat16)

        return base + blocks, (blocks > 0) & more

    lax.fori_loop(0, parts, part_step, (jnp.int32(0), False))


def attend(which, lists, counts, token, queries, pages, first_token=0, suffix=None):
    tokens, width = queries[0].shape
    parts = len(queries)
    page_tokens, kv_width = pages.shape[2:]
    kv_heads = kv_width // HEAD_SIZE
    heads = width // kv_width
    rows = heads * tokens
    vmem = pl.BlockSpec(memory_space=pltpu.VMEM)
    smem = pl.BlockSpec(memory_space=pltpu.SMEM)
    anywhere = pl.BlockSpec(memory_space=pl.ANY)
    extra = () if suffix is None else (suffix,)
    kernel = functools.partial(
        attend_kernel,
        parts=parts,
        kv_heads=kv_heads,
        heads=heads,
        tokens=tokens,
        first_token=first_token,
        suffix=suffix is not None,
    )
    results = pl.pallas_call(
        kernel,
        name="attend_own" if suffix is not None else "attend",
        out_shape=[jax.ShapeDtypeStruct((tokens, width), jnp.bfloat16)] * parts
        + [jax.ShapeDtypeStruct((kv_heads * heads, tokens), jnp.float32)] * parts,
        in_specs=[smem, smem, smem] + [anywhere] * (parts + 2) + [vmem] * len(extra),
        out_specs=[vmem] * (2 * parts),
        scratch_shapes=[
            pltpu.VMEM((parts, tokens, width), jnp.bfloat16),
            pltpu.SemaphoreType.DMA((parts,)),
            pltpu.VMEM((2, pages_per_block, 2, page_tokens, kv_width), jnp.bfloat16),
            pltpu.SemaphoreType.DMA((2, pages_per_block)),
            pltpu.VMEM((kv_heads, rows, HEAD_SIZE), jnp.float32),
            pltpu.VMEM((kv_heads, rows, HEAD_SIZE), jnp.float32),
            pltpu.VMEM((kv_heads, rows, HEAD_SIZE), jnp.float32),
        ],
        cost_estimate=pl.CostEstimate(
            flops=10_000_000_000, bytes_accessed=6_000_000, transcendentals=0
        ),
    )(which, lists, counts, token, *queries, pages, *extra)
    return list(zip(results[:parts], results[parts:]))


def combine_kernel(token, *refs, parts, heads):
    outs, lses = refs[:parts], refs[parts : 2 * parts]
    out, lse = refs[2 * parts :]
    tokens = out.shape[0]
    blank = jnp.full((HEAD_SIZE - heads, tokens), nothing, jnp.float32)
    stats = [jnp.concatenate([x[...], blank], axis=0).T for x in lses]
    top = functools.reduce(jnp.maximum, stats)
    shares = [jnp.exp2(x - top) for x in stats]
    total = functools.reduce(jnp.add, shares)
    shares = [x / total for x in shares]
    lse[...] = (top + jnp.log2(total)).T[:heads]
    for head in range(heads):
        columns = slice(head * HEAD_SIZE, (head + 1) * HEAD_SIZE)
        terms = [
            o[:, columns].astype(jnp.float32) * share[:, head : head + 1]
            for o, share in zip(outs, shares)
        ]
        out[:, columns] = functools.reduce(jnp.add, terms).astype(jnp.bfloat16)


def combine(parts, token):
    tokens, width = parts[0][0].shape
    heads = width // HEAD_SIZE
    vmem = pl.BlockSpec(memory_space=pltpu.VMEM)
    return pl.pallas_call(
        functools.partial(combine_kernel, parts=len(parts), heads=heads),
        name="combine",
        out_shape=(
            jax.ShapeDtypeStruct((tokens, width), jnp.bfloat16),
            jax.ShapeDtypeStruct((heads, tokens), jnp.float32),
        ),
        in_specs=[pl.BlockSpec(memory_space=pl.ANY)] + [vmem] * (2 * len(parts)),
        out_specs=(vmem, vmem),
        cost_estimate=pl.CostEstimate(
            flops=1_000_000_000, bytes_accessed=3_000_000, transcendentals=0
        ),
    )(token, *[p[0] for p in parts], *[p[1] for p in parts])


def page_lists(page_ids, prefix_pages, page_home, pool_rows):
    cache_index = lax.axis_index("cache")
    slots = page_ids.shape[1]
    sent = jnp.concatenate([page_ids, prefix_pages[:, None]], axis=1)
    arrived = lax.all_gather(sent, "cache", axis=0, tiled=True)
    ids, lengths = arrived[:, :slots], arrived[:, slots]
    table = jnp.arange(page_home.shape[0], dtype=jnp.int32)
    rows = jnp.sum(jnp.where(ids[:, :, None] == table, page_home, 0), axis=2)
    within = rows - cache_index * pool_rows
    slot = jnp.arange(slots, dtype=jnp.int32)
    mine = (within >= 0) & (within < pool_rows) & (slot[None, :] < lengths[:, None])
    earlier = slot[:, None] < slot[None, :]
    rank = jnp.sum(jnp.where(earlier[None] & mine[:, :, None], 1, 0), axis=1)
    chosen = mine[:, :, None] & (rank[:, :, None] == slot)
    lists = jnp.sum(jnp.where(chosen, within[:, :, None], 0), axis=1)
    return lists.astype(jnp.int32), jnp.sum(mine, axis=1).astype(jnp.int32)


def place_kernel(source, *refs):
    terms, out = refs[:-1], refs[-1]
    for i, term in enumerate(terms):
        out[source[i]] = term[...]


def place(sources, terms):
    tokens, width = terms[0].shape
    vmem = pl.BlockSpec(memory_space=pltpu.VMEM)
    return pl.pallas_call(
        place_kernel,
        name="place",
        out_shape=jax.ShapeDtypeStruct((len(terms), tokens, width), terms[0].dtype),
        in_specs=[pl.BlockSpec(memory_space=pltpu.SMEM)] + [vmem] * len(terms),
        out_specs=vmem,
    )(jnp.stack(sources), *terms)


def reduce_line(terms, out_blocks):
    count = lax.axis_size("tensor")
    z = lax.axis_index("tensor")

    def chunk(index):
        index = jnp.clip(index, 0, count - 1)
        return lax.dynamic_slice_in_dim(terms, index * out_blocks, out_blocks, 0)

    def add(*parts):
        return functools.reduce(jnp.add, [p.astype(jnp.float32) for p in parts]).astype(terms.dtype)

    up = down = None
    for step in range(1, count):
        up_send, down_send = chunk(count - step + z), chunk(z - (count - step))
        if up is not None:
            up_send, down_send = add(up_send, up), add(down_send, down)
        up = lax.ppermute(up_send, "tensor", [(i, i + 1) for i in range(step)])
        down = lax.ppermute(
            down_send, "tensor", [(count - 1 - i, count - 2 - i) for i in range(step)]
        )
    return add(chunk(z), up, down)


def attention_block(queries, suffix_key_value, kv_pages, page_ids, prefix_pages, page_home, out_weight):
    cache_count = lax.axis_size("cache")
    cache_index = lax.axis_index("cache")
    pool_rows = kv_pages.shape[0]
    chips = cache_count // 2
    chip, core = cache_index // 2, cache_index % 2
    tokens = queries.shape[0] // token_pieces

    def swap(x, chip_shift, other_core):
        pairs = []
        for source in range(cache_count):
            at_chip, at_core = source // 2, source % 2
            at_core = 1 - at_core if other_core else at_core
            pairs.append((source, (at_chip + chip_shift) % chips * 2 + at_core))
        return jax.tree.map(lambda leaf: lax.ppermute(leaf, "cache", pairs), x)

    def device_at(chip_shift, other_core):
        return (chip + chip_shift) % chips * 2 + (1 - core if other_core else core)

    lists, counts = page_lists(page_ids, prefix_pages, page_home, pool_rows)
    queries, lists = lax.optimization_barrier((queries, lists))
    pieces = [queries[i * tokens : (i + 1) * tokens] for i in range(token_pieces)]
    near = [[piece] + [swap(piece, s, False) for s in range(1, chips)] for piece in pieces]

    def attend_pair(piece, s, same, token):
        which = jnp.stack([device_at(-s, False), device_at(-s, True)])
        pair = [same, swap(same, 0, True)]
        return attend(
            which,
            lists,
            counts,
            token,
            pair,
            kv_pages,
            piece * tokens,
            None if s else suffix_key_value,
        )

    def attend_far(piece, token):
        joined = []
        for s, same in enumerate(near[piece][1:], 1):
            mine, theirs = attend_pair(piece, s, same, token)
            theirs = swap(theirs, 0, True)
            joined.append(combine([mine, theirs], token))
        sent = [swap(x, -s, False) for s, x in enumerate(joined, 1)]
        return sent, joined[-1][1]

    def mix(piece, token):
        mine, theirs = own[piece]
        theirs = swap(theirs, 0, True)
        return combine([mine, theirs, *far[piece]], token)

    def terms_of(piece, s):
        block = swap(mixed[piece], s, False) if s else mixed[piece]
        results = []
        for other in (False, True):
            here = swap(block, 0, True) if other else block
            term = jnp.dot(here, out_weight, preferred_element_type=jnp.float32)
            term = term.astype(jnp.bfloat16)
            results.append(swap(term, -s, other) if s or other else term)
        return results

    def reduce_terms(terms):
        sources = [device_at(s, other) for s in range(chips) for other in (False, True)]
        placed = place(sources, terms)
        summed = reduce_line(placed, cache_count // lax.axis_size("tensor"))
        return jnp.concatenate([summed[i] for i in range(summed.shape[0])], axis=1)

    own, far, mixed = {}, {}, {}
    own[0] = attend_pair(0, 0, near[0][0], counts)
    near[0][1:], own[0] = lax.optimization_barrier((near[0][1:], own[0]))
    token = own[0][0][1]
    for piece in range(token_pieces):
        far[piece], token = attend_far(piece, token)
    for piece in range(token_pieces):
        if piece:
            own[piece] = attend_pair(piece, 0, near[piece][0], token)
            token = own[piece][0][1]
        mixed[piece], token = mix(piece, token)
    results = [
        reduce_terms([term for s in range(chips) for term in terms_of(piece, s)])
        for piece in range(token_pieces)
    ]
    return jnp.concatenate(results, axis=0)


def solution(mesh):
    in_specs = (
        P(("groups", "cache"), "tensor"),
        P(None, ("groups", "cache"), "tensor"),
        P(("groups", "cache"), None, None, "tensor"),
        P(("groups", "cache"), None),
        P(("groups", "cache")),
        P("groups"),
        P("tensor", "cache"),
    )
    out_specs = P(("groups", "cache"), "tensor")
    return jax.shard_map(
        attention_block, mesh=mesh, in_specs=in_specs, out_specs=out_specs, check_vma=False
    )
```

```python
import functools

import jax
import jax.numpy as jnp
from jax import lax
from jax.experimental import pallas as pl
from jax.experimental.pallas import tpu as pltpu
from jax.sharding import PartitionSpec as P


HEAD_SIZE = 128

nothing = -1e30
pages_per_block = 4
token_pieces = 2
projection_parts = (1, 2)
log2_e = 1.4426950408889634


def attend_kernel(which, lists, counts, token, *refs, parts, kv_heads, heads, tokens, first_token, suffix):
    queries, refs = refs[:parts], refs[parts:]
    pages, refs = refs[0], refs[1:]
    if suffix:
        suffix_kv, refs = refs[0], refs[1:]
    outs, lses, refs = refs[:parts], refs[parts : 2 * parts], refs[2 * parts :]
    q, q_sems, buf, sems, top_s, sum_s, acc_s = refs
    page_tokens = pages.shape[2]
    rows = heads * tokens
    factor = HEAD_SIZE ** (-0.5) * log2_e
    block_keys = pages_per_block * page_tokens

    def live_of(part):
        return counts[which[part]]

    def blocks_of(part):
        return (live_of(part) + pages_per_block - 1) // pages_per_block

    def copy_of(part, block, slot, place):
        row = lists[which[part], block * pages_per_block + place]
        return pltpu.make_async_copy(pages.at[row], buf.at[slot, place], sems.at[slot, place])

    def start(part, block, slot):
        for place in range(pages_per_block):
            copy_of(part, block, slot, place).start()

    def query_copy(part):
        return pltpu.make_async_copy(queries[part], q.at[part], q_sems.at[part])

    for part in range(parts):
        query_copy(part).start()

    def queries_of(part, kv_head):
        head = kv_head * heads
        return jnp.concatenate(
            [
                q[part, :, (head + i) * HEAD_SIZE : (head + i + 1) * HEAD_SIZE]
                for i in range(heads)
            ],
            axis=0,
        )

    def lane_tiles(x):
        return [x[:, i : i + HEAD_SIZE] for i in range(0, x.shape[1], HEAD_SIZE)]

    def step(part, kv_head, keys, values, mask, first):
        s = lax.dot_general(
            queries_of(part, kv_head),
            keys,
            (((1,), (1,)), ((), ())),
            preferred_element_type=jnp.float32,
        )
        s = mask(s)
        tops = functools.reduce(jnp.maximum, lane_tiles(s))
        top = jnp.broadcast_to(jnp.max(tops, axis=1, keepdims=True), (rows, HEAD_SIZE))
        if not first:
            before = top_s[kv_head]
            top = jnp.maximum(before, top)
            alpha = jnp.exp2((before - top) * factor)
        weights = [jnp.exp2((tile - top) * factor) for tile in lane_tiles(s)]
        sums = functools.reduce(jnp.add, weights)
        product = lax.dot_general(
            jnp.concatenate([w.astype(jnp.bfloat16) for w in weights], axis=1),
            values,
            (((1,), (0,)), ((), ())),
            preferred_element_type=jnp.float32,
        )
        top_s[kv_head] = top
        if first:
            sum_s[kv_head] = sums
            acc_s[kv_head] = product
        else:
            sum_s[kv_head] = sum_s[kv_head] * alpha + sums
            acc_s[kv_head] = acc_s[kv_head] * alpha + product

    def columns_of(kv_head):
        return slice(kv_head * HEAD_SIZE, (kv_head + 1) * HEAD_SIZE)

    def begin_suffix():
        def causal(s):
            token = lax.broadcasted_iota(jnp.int32, s.shape, 0) % tokens + first_token
            key = lax.broadcasted_iota(jnp.int32, s.shape, 1)
            return jnp.where(key <= token, s, nothing)

        keys = slice(0, first_token + tokens)
        for kv_head in range(kv_heads):
            columns = columns_of(kv_head)
            step(0, kv_head, suffix_kv[0, keys, columns], suffix_kv[1, keys, columns], causal, True)

    def begin_empty():
        top_s[...] = jnp.full(top_s.shape, nothing, jnp.float32)
        sum_s[...] = jnp.zeros(sum_s.shape, jnp.float32)
        acc_s[...] = jnp.zeros(acc_s.shape, jnp.float32)

    def part_step(part, carry):
        base, started = carry
        blocks = blocks_of(part)
        after = jnp.minimum(part + 1, parts - 1)
        more = (part + 1 < parts) & (blocks_of(after) > 0)

        @pl.when((blocks > 0) & jnp.logical_not(started))
        def _():
            start(part, 0, lax.rem(base, 2))

        for i in range(parts):

            @pl.when(part == i)
            def _():
                query_copy(i).wait()

        if suffix:
            pl.when(part == 0)(begin_suffix)
            pl.when(part != 0)(begin_empty)
        else:
            begin_empty()

        def block_step(block, carry):
            slot = lax.rem(base + block, 2)
            last = block + 1 == blocks

            @pl.when(jnp.logical_not(last) | more)
            def _():
                start(jnp.where(last, after, part), jnp.where(last, 0, block + 1), 1 - slot)

            for place in range(pages_per_block):
                copy_of(part, block, slot, place).wait()
            key = lax.broadcasted_iota(jnp.int32, (1, block_keys), 1)
            left = (live_of(part) - block * pages_per_block) * page_tokens
            bias = jnp.where(key < left, 0.0, nothing)
            for kv_head in range(kv_heads):
                keys = buf[slot, :, 0, :, columns_of(kv_head)].reshape(block_keys, HEAD_SIZE)
                values = buf[slot, :, 1, :, columns_of(kv_head)].reshape(block_keys, HEAD_SIZE)
                step(part, kv_head, keys, values, lambda s: s + bias, False)
            return carry

        lax.fori_loop(0, blocks, block_step, 0)

        lane = lax.broadcasted_iota(jnp.int32, (tokens, HEAD_SIZE), 1)
        packed = jnp.zeros((tokens, HEAD_SIZE), jnp.float32)
        for kv_head in range(kv_heads):
            total = jnp.sum(sum_s[kv_head], axis=1, keepdims=True)
            any_key = total > 0.0
            safe = jnp.where(any_key, total, 1.0)
            acc_s[kv_head] = acc_s[kv_head] * (1.0 / safe)
            stat = jnp.where(any_key, top_s[kv_head] * factor + jnp.log2(safe), nothing)
            for i in range(heads):
                packed = jnp.where(
                    lane == kv_head * heads + i, stat[i * tokens : (i + 1) * tokens], packed
                )
        packed = packed.T[: kv_heads * heads]
        for i in range(parts):

            @pl.when(part == i)
            def _():
                lses[i][...] = packed
                for kv_head in range(kv_heads):
                    for j in range(heads):
                        head = kv_head * heads + j
                        outs[i][:, head * HEAD_SIZE : (head + 1) * HEAD_SIZE] = acc_s[
                            kv_head, j * tokens : (j + 1) * tokens
                        ].astype(jnp.bfloat16)

        return base + blocks, (blocks > 0) & more

    lax.fori_loop(0, parts, part_step, (jnp.int32(0), False))


def attend(which, lists, counts, token, queries, pages, first_token=0, suffix=None):
    tokens, width = queries[0].shape
    parts = len(queries)
    page_tokens, kv_width = pages.shape[2:]
    kv_heads = kv_width // HEAD_SIZE
    heads = width // kv_width
    rows = heads * tokens
    vmem = pl.BlockSpec(memory_space=pltpu.VMEM)
    smem = pl.BlockSpec(memory_space=pltpu.SMEM)
    anywhere = pl.BlockSpec(memory_space=pl.ANY)
    extra = () if suffix is None else (suffix,)
    kernel = functools.partial(
        attend_kernel,
        parts=parts,
        kv_heads=kv_heads,
        heads=heads,
        tokens=tokens,
        first_token=first_token,
        suffix=suffix is not None,
    )
    results = pl.pallas_call(
        kernel,
        name="attend_own" if suffix is not None else "attend",
        out_shape=[jax.ShapeDtypeStruct((tokens, width), jnp.bfloat16)] * parts
        + [jax.ShapeDtypeStruct((kv_heads * heads, tokens), jnp.float32)] * parts,
        in_specs=[smem, smem, smem] + [anywhere] * (parts + 2) + [vmem] * len(extra),
        out_specs=[vmem] * (2 * parts),
        scratch_shapes=[
            pltpu.VMEM((parts, tokens, width), jnp.bfloat16),
            pltpu.SemaphoreType.DMA((parts,)),
            pltpu.VMEM((2, pages_per_block, 2, page_tokens, kv_width), jnp.bfloat16),
            pltpu.SemaphoreType.DMA((2, pages_per_block)),
            pltpu.VMEM((kv_heads, rows, HEAD_SIZE), jnp.float32),
            pltpu.VMEM((kv_heads, rows, HEAD_SIZE), jnp.float32),
            pltpu.VMEM((kv_heads, rows, HEAD_SIZE), jnp.float32),
        ],
        cost_estimate=pl.CostEstimate(
            flops=10_000_000_000, bytes_accessed=6_000_000, transcendentals=0
        ),
    )(which, lists, counts, token, *queries, pages, *extra)
    return list(zip(results[:parts], results[parts:]))


def combine_kernel(token, *refs, parts, heads):
    outs, lses = refs[:parts], refs[parts : 2 * parts]
    out, lse = refs[2 * parts :]
    tokens = out.shape[0]
    blank = jnp.full((HEAD_SIZE - heads, tokens), nothing, jnp.float32)
    stats = [jnp.concatenate([x[...], blank], axis=0).T for x in lses]
    top = functools.reduce(jnp.maximum, stats)
    shares = [jnp.exp2(x - top) for x in stats]
    total = functools.reduce(jnp.add, shares)
    shares = [x / total for x in shares]
    lse[...] = (top + jnp.log2(total)).T[:heads]
    for head in range(heads):
        columns = slice(head * HEAD_SIZE, (head + 1) * HEAD_SIZE)
        terms = [
            o[:, columns].astype(jnp.float32) * share[:, head : head + 1]
            for o, share in zip(outs, shares)
        ]
        out[:, columns] = functools.reduce(jnp.add, terms).astype(jnp.bfloat16)


def combine(parts, token):
    tokens, width = parts[0][0].shape
    heads = width // HEAD_SIZE
    vmem = pl.BlockSpec(memory_space=pltpu.VMEM)
    return pl.pallas_call(
        functools.partial(combine_kernel, parts=len(parts), heads=heads),
        name="combine",
        out_shape=(
            jax.ShapeDtypeStruct((tokens, width), jnp.bfloat16),
            jax.ShapeDtypeStruct((heads, tokens), jnp.float32),
        ),
        in_specs=[pl.BlockSpec(memory_space=pl.ANY)] + [vmem] * (2 * len(parts)),
        out_specs=(vmem, vmem),
        cost_estimate=pl.CostEstimate(
            flops=1_000_000_000, bytes_accessed=3_000_000, transcendentals=0
        ),
    )(token, *[p[0] for p in parts], *[p[1] for p in parts])


def page_lists(page_ids, prefix_pages, page_home, pool_rows):
    cache_index = lax.axis_index("cache")
    slots = page_ids.shape[1]
    sent = jnp.concatenate([page_ids, prefix_pages[:, None]], axis=1)
    arrived = lax.all_gather(sent, "cache", axis=0, tiled=True)
    ids, lengths = arrived[:, :slots], arrived[:, slots]
    table = jnp.arange(page_home.shape[0], dtype=jnp.int32)
    rows = jnp.sum(jnp.where(ids[:, :, None] == table, page_home, 0), axis=2)
    within = rows - cache_index * pool_rows
    slot = jnp.arange(slots, dtype=jnp.int32)
    mine = (within >= 0) & (within < pool_rows) & (slot[None, :] < lengths[:, None])
    earlier = slot[:, None] < slot[None, :]
    rank = jnp.sum(jnp.where(earlier[None] & mine[:, :, None], 1, 0), axis=1)
    chosen = mine[:, :, None] & (rank[:, :, None] == slot)
    lists = jnp.sum(jnp.where(chosen, within[:, :, None], 0), axis=1)
    return lists.astype(jnp.int32), jnp.sum(mine, axis=1).astype(jnp.int32)


def place_kernel(position, *refs):
    terms, kept, sent = refs[:-2], refs[-2], refs[-1]
    half = len(terms) // 2
    for i, term in enumerate(terms):
        at = position[i]

        @pl.when(at < half)
        def _():
            kept[at] = term[...]

        @pl.when(at >= half)
        def _():
            sent[at - half] = term[...]


def place(positions, terms):
    tokens, width = terms[0].shape
    vmem = pl.BlockSpec(memory_space=pltpu.VMEM)
    half = jax.ShapeDtypeStruct((len(terms) // 2, tokens, width), terms[0].dtype)
    return pl.pallas_call(
        place_kernel,
        name="place",
        out_shape=(half, half),
        in_specs=[pl.BlockSpec(memory_space=pltpu.SMEM)] + [vmem] * len(terms),
        out_specs=(vmem, vmem),
    )(jnp.stack(positions), *terms)


def halving_position(source, per_chunk, count, index):
    relative = (source // per_chunk) ^ index
    reverse, bit = 0, 1
    while bit < count:
        reverse = reverse * 2 + relative % 2
        relative, bit = relative // 2, bit * 2
    return reverse * per_chunk + source % per_chunk


def reduce_halving(kept, sent):
    count = lax.axis_size("tensor")
    distance = 1
    kept = kept.astype(jnp.float32)
    while distance < count:
        arrived = lax.ppermute(sent, "tensor", [(i, i ^ distance) for i in range(count)])
        distance *= 2
        kept = kept + arrived.astype(jnp.float32)
        if distance < count:
            half = kept.shape[0] // 2
            kept, sent = kept[:half], kept[half:].astype(sent.dtype)
    return kept.astype(sent.dtype)


def attention_block(queries, suffix_key_value, kv_pages, page_ids, prefix_pages, page_home, out_weight):
    cache_count = lax.axis_size("cache")
    cache_index = lax.axis_index("cache")
    pool_rows = kv_pages.shape[0]
    chips = cache_count // 2
    chip, core = cache_index // 2, cache_index % 2
    tokens = queries.shape[0] // token_pieces

    def swap(x, chip_shift, other_core):
        pairs = []
        for source in range(cache_count):
            at_chip, at_core = source // 2, source % 2
            at_core = 1 - at_core if other_core else at_core
            pairs.append((source, (at_chip + chip_shift) % chips * 2 + at_core))
        return jax.tree.map(lambda leaf: lax.ppermute(leaf, "cache", pairs), x)

    def device_at(chip_shift, other_core):
        return (chip + chip_shift) % chips * 2 + (1 - core if other_core else core)

    lists, counts = page_lists(page_ids, prefix_pages, page_home, pool_rows)
    queries, lists = lax.optimization_barrier((queries, lists))
    pieces = [queries[i * tokens : (i + 1) * tokens] for i in range(token_pieces)]
    near = [[piece] + [swap(piece, s, False) for s in range(1, chips)] for piece in pieces]

    def attend_pair(piece, s, same, token):
        which = jnp.stack([device_at(-s, False), device_at(-s, True)])
        pair = [same, swap(same, 0, True)]
        return attend(
            which,
            lists,
            counts,
            token,
            pair,
            kv_pages,
            piece * tokens,
            None if s else suffix_key_value,
        )

    def attend_far(piece, token):
        joined = []
        for s, same in enumerate(near[piece][1:], 1):
            mine, theirs = attend_pair(piece, s, same, token)
            theirs = swap(theirs, 0, True)
            joined.append(combine([mine, theirs], token))
        sent = [swap(x, -s, False) for s, x in enumerate(joined, 1)]
        return sent, joined[-1][1]

    def mix(piece, token):
        mine, theirs = own[piece]
        theirs = swap(theirs, 0, True)
        return combine([mine, theirs, *far[piece]], token)

    far_blocks, core_blocks = {}, {}

    def block_of(piece, s, other):
        if (piece, s) not in far_blocks:
            here = swap(mixed[piece], s, False) if s else mixed[piece]
            far_blocks[piece, s] = here
            core_blocks[piece, s] = swap(here, 0, True)
        return core_blocks[piece, s] if other else far_blocks[piece, s]

    def term_of(piece, part, s, other):
        rows = tokens // projection_parts[piece]
        here = block_of(piece, s, other)[part * rows : (part + 1) * rows]
        term = jnp.dot(here, out_weight, preferred_element_type=jnp.float32)
        term = term.astype(jnp.bfloat16)
        return swap(term, -s, other) if s or other else term

    def reduce_part(piece, part):
        order = [(s, other) for s in range(chips) for other in (False, True)]
        terms = [term_of(piece, part, s, other) for s, other in order]
        count, index = lax.axis_size("tensor"), lax.axis_index("tensor")
        per_chunk = cache_count // count
        positions = [
            halving_position(device_at(s, other), per_chunk, count, index) for s, other in order
        ]
        kept, sent = place(positions, terms)
        summed = reduce_halving(kept, sent)
        return jnp.concatenate([summed[i] for i in range(summed.shape[0])], axis=1)

    own, far, mixed = {}, {}, {}
    own[0] = attend_pair(0, 0, near[0][0], counts)
    near[0][1:], own[0] = lax.optimization_barrier((near[0][1:], own[0]))
    token = own[0][0][1]
    for piece in range(token_pieces):
        far[piece], token = attend_far(piece, token)
    for piece in range(token_pieces):
        if piece:
            own[piece] = attend_pair(piece, 0, near[piece][0], token)
            token = own[piece][0][1]
        mixed[piece], token = mix(piece, token)
    results = [
        reduce_part(piece, part)
        for piece in range(token_pieces)
        for part in range(projection_parts[piece])
    ]
    return jnp.concatenate(results, axis=0)


def solution(mesh):
    in_specs = (
        P(("groups", "cache"), "tensor"),
        P(None, ("groups", "cache"), "tensor"),
        P(("groups", "cache"), None, None, "tensor"),
        P(("groups", "cache"), None),
        P(("groups", "cache")),
        P("groups"),
        P("tensor", "cache"),
    )
    out_specs = P(("groups", "cache"), "tensor")
    return jax.shard_map(
        attention_block, mesh=mesh, in_specs=in_specs, out_specs=out_specs, check_vma=False
    )
```
